128 devices in a mesh: section: 32 (over y, x, core), tp: 4 (over z).
Axes of the slice: x: 4, y: 4, z: 4, core: 2. Of those that a mesh axis runs over, the one named last changes fastest.
Arguments:
- tokens_in: bfloat16 [2, 224, 7168], P(None, None, 'tp'), may hold values from -6 to 6
- norm_gain: float32 [2, 7168], P(None, 'tp'), may hold values from 0.5 to 2
- router_weight: float32 [2, 7168], P(None, 'tp'), may hold values from -0.0625 to 0.0625
- gate_weight: bfloat16 [32, 7168, 1152], P('section', 'tp'), may hold values from -0.0625 to 0.0625
- up_weight: bfloat16 [32, 7168, 1152], P('section', 'tp'), may hold values from -0.0625 to 0.0625
- down_weight: bfloat16 [32, 1152, 7168], P('section', None, 'tp'), may hold values from -0.046875 to 0.046875
- routed_rows: int32 [2, 2, 112], replicated, may hold values from 0 to 223, as said below
- routed_count: int32 [2, 2], replicated, may hold values from 56 to 112, as said below
Outputs:
- tokens_out: bfloat16 [2, 224, 7168], P(None, 'section', 'tp')
The draws below stay inside these ranges and needn't reach their ends.
Inputs may be any that keep to these rules, and one draw needn't show every extreme that they name: `routed_rows`: within each microbatch and layer, the 112 entries are distinct token positions. Only the leading routed_count entries of a list are live; some list is full in every draw.
All inputs are finite; a program needn't handle non-finite values.
Results may differ from the reference program's by a relative error of at most 0.0074.
Values may be sent and summed in bfloat16 or wider, within the bound.
A program may use at most 64 MiB of HBM per device.

```python
import math
import jax
import jax.numpy as jnp
from jax import lax

D = 7168
FF = 18432
MB_TOKENS = 224
MICRO = 2
LAYERS = 2
HIDDEN_PARTS = 16
CAPACITY = 112


def draw_routed_rows(key, part):
    subkeys = jax.random.split(jax.random.fold_in(key, 11), MICRO * LAYERS)
    orders = jax.vmap(lambda subkey: jax.random.permutation(subkey, MB_TOKENS))(subkeys)
    return orders[:, :CAPACITY].reshape(MICRO, LAYERS, CAPACITY).astype(jnp.int32)


def draw_routed_count(key, part):
    drawn = jax.random.randint(jax.random.fold_in(key, 21), (MICRO * LAYERS,), CAPACITY // 2, CAPACITY + 1)
    position = jax.random.randint(jax.random.fold_in(key, 22), (), 0, MICRO * LAYERS)
    flattened = jnp.where(jnp.arange(MICRO * LAYERS) == position, CAPACITY, drawn)
    return flattened.reshape(MICRO, LAYERS).astype(jnp.int32)


def levels(own_key, dims, shards, smallest, top_value):
    def one(dim, parts):
        heights = jax.random.uniform(jax.random.fold_in(jax.random.fold_in(own_key, 6), dim), (parts,), jnp.float32, smallest / len(shards), top_value / len(shards))
        return jnp.repeat(jnp.exp(heights), dims[dim] // parts).reshape((-1,) + (1,) * (len(dims) - dim - 1))

    level = one(*shards[0])
    for cut in shards[1:]:
        level = level * one(*cut)
    return level


def noise(key, extent, scale, most, cuts=(), held_as=jnp.bfloat16):
    result = scale * jax.random.normal(key, extent, jnp.float32)
    if cuts:
        result = result * levels(key, extent, cuts, -0.22, 0.18)
    return jnp.clip(result, -most, most).astype(held_as)


def setup_inputs(seed: int = 0) -> dict:
    streams_of = jax.random.split(jax.random.key(seed), 9)
    tokens_in = noise(streams_of[0], (MICRO, MB_TOKENS, D), 1.0, 6.0, ((2, 4),))
    norm_gain = jnp.clip(jnp.exp(math.log(2.0) - 1.3862944 * jax.random.uniform(streams_of[1], (LAYERS, D), jnp.float32) ** levels(streams_of[1], (LAYERS, D), ((1, 4),), -0.2, 0.2)), 0.5, 2.0)
    router_weight = noise(streams_of[2], (LAYERS, D), D ** -0.5, 0.0625, ((1, 4),), jnp.float32)
    gate_weight = noise(streams_of[3], (LAYERS * HIDDEN_PARTS, D, FF // HIDDEN_PARTS), D ** -0.5, 0.0625, ((0, 32), (1, 4)))
    up_weight = noise(streams_of[4], (LAYERS * HIDDEN_PARTS, D, FF // HIDDEN_PARTS), D ** -0.5, 0.0625, ((0, 32), (1, 4)))
    down_weight = noise(streams_of[5], (LAYERS * HIDDEN_PARTS, FF // HIDDEN_PARTS, D), FF ** -0.5, 0.046875, ((0, 32), (2, 4)))
    routed_rows = draw_routed_rows(jax.random.fold_in(streams_of[8], 71), 0)
    routed_count = draw_routed_count(jax.random.fold_in(streams_of[8], 71), 0)
    return {"tokens_in": tokens_in, "norm_gain": norm_gain, "router_weight": router_weight, "gate_weight": gate_weight, "up_weight": up_weight, "down_weight": down_weight, "routed_rows": routed_rows, "routed_count": routed_count}


EPSILON = 1e-06

def run_layer(stream, routed_ids, live_count, gain_row, router_row, gate_full, up_full, down_full):
    picked = stream[routed_ids]
    floats = picked.astype(jnp.float32)
    squares = lax.optimization_barrier(jnp.sum(floats * floats, axis=1))
    logits = lax.optimization_barrier(jnp.sum(floats * router_row, axis=1))
    inverse = lax.rsqrt(squares / D + EPSILON)[:, None]
    scaled = (floats * gain_row).astype(jnp.bfloat16)
    gate = jnp.dot(scaled, gate_full, preferred_element_type=jnp.float32) * inverse
    up_values = jnp.dot(scaled, up_full, preferred_element_type=jnp.float32) * inverse
    hidden = (jax.nn.silu(gate) * up_values).astype(jnp.bfloat16)
    output = jnp.dot(hidden, down_full, preferred_element_type=jnp.float32)
    router_gate = jax.nn.sigmoid(logits)[:, None]
    updated = (floats + router_gate * output).astype(jnp.bfloat16)
    is_live = jnp.arange(routed_ids.shape[0], dtype=jnp.int32) < live_count
    new_rows = jnp.where(is_live[:, None], updated, picked)
    return stream.at[routed_ids].set(new_rows)

def reference(tokens_in, norm_gain, router_weight, gate_weight, up_weight, down_weight, routed_rows, routed_count):
    streams = tokens_in
    for layer_index in range(LAYERS):
        first = layer_index * HIDDEN_PARTS
        last = first + HIDDEN_PARTS
        gate_full = jnp.transpose(gate_weight[first:last], (1, 0, 2)).reshape(D, FF)
        up_full = jnp.transpose(up_weight[first:last], (1, 0, 2)).reshape(D, FF)
        down_full = down_weight[first:last].reshape(FF, D)
        streams = jax.vmap(run_layer, in_axes=(0, 0, 0, None, None, None, None, None))(streams, routed_rows[:, layer_index], routed_count[:, layer_index], norm_gain[layer_index], router_weight[layer_index], gate_full, up_full, down_full)
    return streams
```

```python
import jax
import jax.numpy as jnp
from jax import lax
from jax.experimental import pallas as pl
from jax.experimental.pallas import tpu as pltpu
from jax.sharding import PartitionSpec as P

MESH = pl.DeviceIdType.MESH
F32 = jnp.float32
BF16 = jnp.bfloat16

MICRO = 2
CAP = 112
TOK = 224
Q = 1792
HID = 1152
D = 7168
EPSILON = 1e-06
ROWS = 128
HALF = Q // 2
BLOCKS = HALF // 128
OWN_TOKENS = 7
CHUNKS = ((0, 512), (512, 640))


def iota(shape, dim):
    return lax.broadcasted_iota(jnp.int32, shape, dim)


def onehot(hit):
    return jnp.where(hit, 1.0, 0.0).astype(BF16)


def padded_column(row, fill):
    r, c = iota((ROWS, CAP), 0), iota((ROWS, CAP), 1)
    hit = (c == r - 4 * (r >> 5)) & ((r & 31) < 28)
    column = jnp.sum(jnp.where(hit, row, 0.0), axis=1, keepdims=True)
    return jnp.where((iota((ROWS, 1), 0) & 31) < 28, column, fill)


def as_row(column):
    n = column.shape[0]
    eye = iota((n, n), 0) == iota((n, n), 1)
    return jnp.sum(jnp.where(eye, column, 0.0), axis=0, keepdims=True)


def as_column(row, first, n):
    hit = iota((n, ROWS), 1) == iota((n, ROWS), 0) + first
    return jnp.sum(jnp.where(hit, row, 0.0), axis=1, keepdims=True)


def dot(a, b):
    return jnp.dot(a, b, preferred_element_type=F32)


def body(
    tok_h, gain_h, router_h, wg_h, wu_h, wd_h, rows_h, cnt_h,
    out_ref,
    tok, gain, router, wg, wu, wd, rows, cnt,
    picked, scaled, stat, stat_in, part, relay, ring, back, hidden, xcore, xcore_in, keep,
    summed, summed_in, updated, blocks, final, ready, final_in,
    load_sem, stat_s, stat_r, relay_s, relay_r, ring_s, ring_r, back_s, back_r, hid_s, hid_r,
    core_s, core_r, sum_s, sum_r, hop_s, blk_s, fwd_s, blk_r, fin_s, fin_r,
):
    sec = lax.axis_index("section")
    tp = lax.axis_index("tp")
    core = lax.rem(sec, 2)
    group = sec // 16
    chip = lax.rem(sec, 16) // 2
    ahead = lax.rem(tp + 1 + 2 * core, 4)
    behind = lax.rem(tp + 3 + 2 * core, 4)
    across = lax.rem(tp + 2, 4)
    sibling = sec + 1 - 2 * core
    sections, tps = 32, 4

    barrier = pltpu.get_barrier_semaphore()

    @pl.loop(1, sections)
    def _(k):
        pl.semaphore_signal(
            barrier, inc=1, device_id={"section": lax.rem(sec + k, sections), "tp": tp}, device_id_type=MESH
        )

    for k in range(1, tps):
        pl.semaphore_signal(
            barrier, inc=1, device_id={"section": sec, "tp": lax.rem(tp + k, tps)}, device_id_type=MESH
        )

    loads = []

    def load(src, dst):
        copy = pltpu.make_async_copy(src, dst, load_sem.at[len(loads)])
        copy.start()
        loads.append(copy)
        return copy

    small = [load(rows_h, rows), load(cnt_h, cnt), load(gain_h, gain), load(router_h, router)]
    tok_load = [load(tok_h.at[m], tok.at[m]) for m in range(MICRO)]
    wgu_load = []
    for start, n in CHUNKS:
        cols = pl.ds(start, n)
        wgu_load.append(
            (load(wg_h.at[0, :, cols], wg.at[:, cols]), load(wu_h.at[0, :, cols], wu.at[:, cols]))
        )
    wd_load = load(wd_h.at[0], wd)

    sends = []

    def remote(src, dst, ss, rs, section=None, z=None):
        return pltpu.make_async_remote_copy(
            src_ref=src,
            dst_ref=dst,
            send_sem=ss,
            recv_sem=rs,
            device_id={"section": sec if section is None else section, "tp": tp if z is None else z},
            device_id_type=MESH,
        )

    def send(copy):
        copy.start()
        sends.append((None, copy))

    def routed(m, k):
        ids = rows[m, k : k + 1, :].astype(F32)
        count = cnt[m : m + 1, k : k + 1]
        return ids, iota((1, CAP), 1) < count

    def pick(m):
        for copy in small if m == 0 else []:
            copy.wait()
        tok_load[m].wait()

        @pl.when(group == 0)
        def _():
            ids, _ = routed(m, 0)
            column = padded_column(ids, -1.0)
            old = onehot(column == iota((ROWS, TOK), 1).astype(F32))
            for b in range(Q // 256):
                cols = pl.ds(256 * b, 256)
                picked[m, :, cols] = dot(old, tok[m, :, cols]).astype(BF16)

        @pl.when(group == 1)
        def _():
            ids1, _ = routed(m, 1)
            column = padded_column(ids1, -1.0)
            ids0, live0 = routed(m, 0)
            row0 = as_row(padded_column(jnp.where(live0, ids0, -2.0), -2.0))
            hit = column == row0
            is_new = jnp.sum(jnp.where(hit, 1.0, 0.0), axis=1, keepdims=True) > 0.5
            new = onehot(hit)
            old = onehot((column == iota((ROWS, TOK), 1).astype(F32)) & ~is_new)
            for b in range(2 * BLOCKS):
                cols = pl.ds(128 * b, 128)
                picked[m, :, cols] = (dot(old, tok[m, :, cols]) + dot(new, blocks[m, b])).astype(BF16)

        squares = jnp.zeros((ROWS, 256), F32)
        logits = jnp.zeros((ROWS, 256), F32)
        for b in range(Q // 256):
            cols = pl.ds(256 * b, 256)
            values = picked[m, :, cols].astype(F32)
            squares = squares + values * values
            logits = logits + values * router[pl.ds(group, 1), cols]
            scaled[m, :, cols] = (values * gain[pl.ds(group, 1), cols]).astype(BF16)
        squares = as_row(jnp.sum(squares, axis=1, keepdims=True))
        logits = as_row(jnp.sum(logits, axis=1, keepdims=True))
        which = iota((8, ROWS), 0)
        stat[m] = jnp.where(which == 0, squares, jnp.where(which == 1, logits, 0.0))

    def stat_copy(m, k):
        return remote(stat.at[m], stat_in.at[m, k - 1], stat_s.at[m, k - 1], stat_r.at[m, k - 1], z=lax.rem(tp + k, tps))

    def send_stats(m):
        for k in range(1, tps):
            send(stat_copy(m, k))

    def spans(n):
        start, width = CHUNKS[n]
        return pl.ds(2 * start, 2 * width), 2 * start, width

    def relay_copy(m, n):
        cols = spans(n)[0]
        return remote(part.at[m, across, :, cols], relay.at[m, :, cols], relay_s.at[m, n], relay_r.at[m, n], z=ahead)

    def back_copy(m, n):
        cols = spans(n)[0]
        return remote(part.at[m, behind, :, cols], back.at[m, :, cols], back_s.at[m, n], back_r.at[m, n], z=behind)

    def ring_copy(m, n):
        cols = spans(n)[0]
        return remote(ring.at[m, 0, :, cols], ring.at[m, 1, :, cols], ring_s.at[m, n], ring_r.at[m, n], z=ahead)

    def project(m, n):
        start, width = CHUNKS[n]
        if m == 0:
            wgu_load[n][0].wait()
        x = scaled[m]
        gate = dot(x, wg[:, start : start + width]).astype(BF16)
        part[m, :, :, 2 * start : 2 * start + width] = gate.reshape(tps, 32, width)
        if m == 0:
            wgu_load[n][1].wait()
        up = dot(x, wu[:, start : start + width]).astype(BF16)
        part[m, :, :, 2 * start + width : 2 * start + 2 * width] = up.reshape(tps, 32, width)
        if n == 0:
            send_stats(m)
        send(relay_copy(m, n))
        send(back_copy(m, n))

    def pass_on(m, n):
        cols = spans(n)[0]
        relay_copy(m, n).wait_recv()
        ring[m, 0, :, cols] = (part[m, ahead, :, cols].astype(F32) + relay[m, :, cols].astype(F32)).astype(BF16)
        send(ring_copy(m, n))

    def total_stats(m):
        return stat[m] + stat_in[m, 0] + stat_in[m, 1] + stat_in[m, 2]

    def hidden_copy(m, n, k):
        start, width = CHUNKS[n]
        mine = hidden.at[m, tp, :, pl.ds(start, width)]
        return remote(mine, mine, hid_s.at[m, n, k - 1], hid_r.at[m, n, k - 1], z=lax.rem(tp + k, tps))

    def activate(m, n):
        cols, first, width = spans(n)
        start = CHUNKS[n][0]
        if n == 0:
            for k in range(1, tps):
                stat_copy(m, k).wait_recv()
        back_copy(m, n).wait_recv()
        ring_copy(m, n).wait_recv()
        inverse = lax.rsqrt(as_column(total_stats(m)[0:1], 32 * tp, 32) / D + EPSILON)

        def values(at):
            c = pl.ds(at, width)
            return part[m, tp, :, c].astype(F32) + back[m, :, c].astype(F32) + ring[m, 1, :, c].astype(F32)

        gate = values(first) * inverse
        up = values(first + width) * inverse
        hidden[m, tp, :, start : start + width] = (gate / (1.0 + jnp.exp(-gate)) * up).astype(BF16)
        for k in (2, 1, 3):
            send(hidden_copy(m, n, k))

    def core_copy(m):
        return remote(xcore.at[m], xcore_in.at[m], core_s.at[m], core_r.at[m], section=sibling)

    def down(m):
        for n in range(len(CHUNKS)):
            for k in range(1, tps):
                hidden_copy(m, n, k).wait_recv()
        if m == 0:
            wd_load.wait()
        x = hidden[m].reshape(ROWS, HID)
        theirs = pl.ds(pl.multiple_of(HALF * (1 - core), 128), HALF)
        xcore[m] = dot(x, wd[:, theirs]).astype(BF16)
        send(core_copy(m))
        mine = pl.ds(pl.multiple_of(HALF * core, 128), HALF)
        keep[m] = dot(x, wd[:, mine])

    def sum_copy(m, k):
        there = lax.rem(chip + k, 8)
        return there < BLOCKS, remote(
            summed.at[m, there], summed_in.at[m, k - 1], sum_s.at[m, k - 1], sum_r.at[m, k - 1],
            section=16 * group + 2 * there + core,
        )

    def send_if(condition, copy):
        @pl.when(condition)
        def _():
            copy.start()

        sends.append((condition, copy))

    def spread(m):
        core_copy(m).wait_recv()
        for b in range(BLOCKS):
            cols = pl.ds(128 * b, 128)
            summed[m, b] = (keep[m, :, cols] + xcore_in[m, :, cols].astype(F32)).astype(BF16)
        for k in range(1, 8):
            there = lax.rem(chip + k, 8)

            @pl.when(there < BLOCKS)
            def _():
                sum_copy(m, k)[1].start()

            sends.append((there < BLOCKS, sum_copy(m, k)[1]))

    owner = chip < BLOCKS
    my_block = BLOCKS * core + chip
    my_columns = pl.ds(pl.multiple_of(128 * jnp.minimum(my_block, 2 * BLOCKS - 1), 128), 128)

    def hop_copy(m):
        return remote(
            updated.at[m], blocks.at[m, my_block], hop_s.at[m], blk_r.at[m, my_block],
            section=16 + 2 * lax.rem(chip + 4, 8) + core,
        )

    def combine(m):
        @pl.when(owner)
        def _():
            total = summed[m, chip].astype(F32)
            for k in range(1, 8):
                sum_copy(m, k)[1].wait_recv()
                total = total + summed_in[m, k - 1].astype(F32)
            logits = as_column(total_stats(m)[1:2], 0, ROWS)
            gate = 1.0 / (1.0 + jnp.exp(-logits))
            updated[m] = (picked[m, :, my_columns].astype(F32) + gate * total).astype(BF16)

            @pl.when(group == 0)
            def _():
                hop_copy(m).start()

        sends.append((owner & (group == 0), hop_copy(m)))

    source = lax.rem(chip + 4, 8)
    has_block = source < BLOCKS

    def block_copy(m, k):
        block = BLOCKS * core + source
        return remote(
            blocks.at[m, block], blocks.at[m, block], blk_s.at[m, k - 1], blk_r.at[m, block],
            section=16 + 2 * lax.rem(chip + k, 8) + core,
        )

    def forward_copy(m, k):
        block = BLOCKS * core + lax.rem(source + k, 8)
        return remote(
            blocks.at[m, block], blocks.at[m, block], fwd_s.at[m, k], blk_r.at[m, block], section=sibling
        )

    def arrival(m, block):
        return remote(blocks.at[m, block], blocks.at[m, block], fwd_s.at[m, 0], blk_r.at[m, block], section=sibling)

    def broadcast(m):
        @pl.when((group == 1) & has_block)
        def _():
            arrival(m, BLOCKS * core + source).wait_recv()
            for k in range(1, 8):
                block_copy(m, k).start()
            forward_copy(m, 0).start()

        for k in range(1, 8):
            sends.append(((group == 1) & has_block, block_copy(m, k)))
        sends.append(((group == 1) & has_block, forward_copy(m, 0)))

    def forward(m):
        @pl.when(group == 1)
        def _():
            for k in (1, 7, 4, 5, 3, 2, 6):
                there = lax.rem(source + k, 8)

                @pl.when(there < BLOCKS)
                def _():
                    arrival(m, BLOCKS * core + there).wait_recv()
                    forward_copy(m, k).start()

            for b in range(BLOCKS):
                arrival(m, BLOCKS * (1 - core) + b).wait_recv()

        for k in range(1, 8):
            sends.append(((group == 1) & (lax.rem(source + k, 8) < BLOCKS), forward_copy(m, k)))

    finisher = owner & (group == 1)

    def finish(m):
        @pl.when(finisher)
        def _():
            r = iota((16 * sections, 1), 0)
            i = r & 7
            token = jnp.where((((r >> 3) & 1) == m) & (i < OWN_TOKENS), OWN_TOKENS * (r >> 4) + i, -5).astype(F32)

            def matches(k):
                ids, live = routed(m, k)
                return token == as_row(padded_column(jnp.where(live, ids, -1.0), -1.0))

            def any_of(hit):
                return jnp.sum(jnp.where(hit, 1.0, 0.0), axis=1, keepdims=True) > 0.5

            last = matches(1)
            in_last = any_of(last)
            first = matches(0)
            in_first = any_of(first)
            base = token == iota((16 * sections, TOK), 1).astype(F32)
            value = (
                dot(onehot(base & ~(in_first | in_last)), tok[m, :, my_columns])
                + dot(onehot(first & ~in_last), blocks[m, my_block])
                + dot(onehot(last), updated[m])
            )
            if m == 0:
                final[...] = value
            else:
                ready[...] = (final[...] + value).astype(BF16).reshape(sections, 16, 128)

    def final_copy(k):
        there = lax.rem(sec + k, sections)
        return remote(ready.at[there], final_in.at[my_block], fin_s.at[k - 1], fin_r.at[my_block], section=there)

    def deliver():
        @pl.when(finisher)
        def _():
            @pl.loop(1, sections)
            def _(k):
                final_copy(k).start()

            final_in[my_block] = ready[sec]

        for b in range(2 * BLOCKS):

            @pl.when(jnp.logical_not(finisher & (my_block == b)))
            def _():
                remote(ready.at[0], final_in.at[b], fin_s.at[0], fin_r.at[b], section=sibling).wait_recv()

            for m in range(MICRO):
                out_ref[m, :, 128 * b : 128 * b + 128] = final_in[b, 8 * m : 8 * m + OWN_TOKENS, :]

    pl.semaphore_wait(barrier, sections + tps - 2)
    broadcast(0)
    forward(0)
    pick(0)
    project(0, 0)
    project(0, 1)
    pass_on(0, 0)
    pass_on(0, 1)
    activate(0, 0)
    broadcast(1)
    forward(1)
    pick(1)
    project(1, 0)
    activate(0, 1)
    project(1, 1)
    pass_on(1, 0)
    pass_on(1, 1)
    down(0)
    activate(1, 0)
    spread(0)
    activate(1, 1)
    combine(0)
    down(1)
    spread(1)
    finish(0)
    combine(1)
    finish(1)
    deliver()

    for condition, copy in sends:
        if condition is None:
            copy.wait_send()
        else:
            pl.when(condition)(copy.wait_send)

    @pl.when(finisher)
    def _():
        @pl.loop(1, sections)
        def _(k):
            final_copy(k).wait_send()


def on_device(*args):
    dma = pltpu.SemaphoreType.DMA
    n = len(CHUNKS)
    return pl.pallas_call(
        body,
        out_shape=jax.ShapeDtypeStruct((MICRO, OWN_TOKENS, Q), BF16),
        in_specs=[pl.BlockSpec(memory_space=pl.ANY)] * 8,
        out_specs=pl.BlockSpec(memory_space=pltpu.VMEM),
        scratch_shapes=[
            pltpu.VMEM((MICRO, TOK, Q), BF16),
            pltpu.VMEM((2, Q), F32),
            pltpu.VMEM((2, Q), F32),
            pltpu.VMEM((Q, HID), BF16),
            pltpu.VMEM((Q, HID), BF16),
            pltpu.VMEM((HID, Q), BF16),
            pltpu.VMEM((MICRO, 2, CAP), jnp.int32),
            pltpu.VMEM((MICRO, 2), jnp.int32),
            pltpu.VMEM((MICRO, ROWS, Q), BF16),
            pltpu.VMEM((MICRO, ROWS, Q), BF16),
            pltpu.VMEM((MICRO, 8, ROWS), F32),
            pltpu.VMEM((MICRO, 3, 8, ROWS), F32),
            pltpu.VMEM((MICRO, 4, 32, 2 * HID), BF16),
            pltpu.VMEM((MICRO, 32, 2 * HID), BF16),
            pltpu.VMEM((MICRO, 2, 32, 2 * HID), BF16),
            pltpu.VMEM((MICRO, 32, 2 * HID), BF16),
            pltpu.VMEM((MICRO, 4, 32, HID), BF16),
            pltpu.VMEM((MICRO, ROWS, HALF), BF16),
            pltpu.VMEM((MICRO, ROWS, HALF), BF16),
            pltpu.VMEM((MICRO, ROWS, HALF), F32),
            pltpu.VMEM((MICRO, 8, ROWS, 128), BF16),
            pltpu.VMEM((MICRO, 7, ROWS, 128), BF16),
            pltpu.VMEM((MICRO, ROWS, 128), BF16),
            pltpu.VMEM((MICRO, 2 * BLOCKS + 1, ROWS, 128), BF16),
            pltpu.VMEM((512, 128), F32),
            pltpu.VMEM((32, 16, 128), BF16),
            pltpu.VMEM((2 * BLOCKS + 1, 16, 128), BF16),
            dma((6 + 2 * n + 1,)),
            dma((MICRO, 3)), dma((MICRO, 3)),
            dma((MICRO, n)), dma((MICRO, n)),
            dma((MICRO, n)), dma((MICRO, n)),
            dma((MICRO, n)), dma((MICRO, n)),
            dma((MICRO, n, 3)), dma((MICRO, n, 3)),
            dma((MICRO,)), dma((MICRO,)),
            dma((MICRO, 7)), dma((MICRO, 7)),
            dma((MICRO,)),
            dma((MICRO, 7)),
            dma((MICRO, 8)),
            dma((MICRO, 2 * BLOCKS + 1)),
            dma((31,)),
            dma((2 * BLOCKS + 1,)),
        ],
        compiler_params=pltpu.CompilerParams(
            collective_id=0, has_side_effects=True, vmem_limit_bytes=60 * 1024 * 1024
        ),
        name="layers",
    )(*args)


def solution(mesh):
    return jax.shard_map(
        on_device,
        mesh=mesh,
        in_specs=(
            P(None, None, "tp"),
            P(None, "tp"),
            P(None, "tp"),
            P("section", "tp", None),
            P("section", "tp", None),
            P("section", None, "tp"),
            P(),
            P(),
        ),
        out_specs=P(None, "section", "tp"),
        check_vma=False,
    )
```

```python
import functools

import jax
import jax.numpy as jnp
from jax import lax
from jax.experimental import pallas as pl
from jax.experimental.pallas import tpu as pltpu
from jax.sharding import PartitionSpec as P

MESH = pl.DeviceIdType.MESH
F32 = jnp.float32
BF16 = jnp.bfloat16

MICRO = 2
CAP = 112
TOK = 224
Q = 1792
HID = 1152
D = 7168
EPSILON = 1e-06
GROUP = 32
HALF = Q // 2
BLOCKS = HALF // 128
OWN_TOKENS = 7
CHUNKS = ((0, 512), (512, 640))


def iota(shape, dim):
    return lax.broadcasted_iota(jnp.int32, shape, dim)


def onehot(hit):
    return jnp.where(hit, 1.0, 0.0).astype(BF16)


def as_row(column):
    n = column.shape[0]
    eye = iota((n, n), 0) == iota((n, n), 1)
    return jnp.sum(jnp.where(eye, column, 0.0), axis=0, keepdims=True)


def as_column(row, first=0, n=CAP):
    hit = iota((n, CAP), 1) == iota((n, CAP), 0) + first
    return jnp.sum(jnp.where(hit, row, 0.0), axis=1, keepdims=True)


def dot(a, b):
    return jnp.dot(a, b, preferred_element_type=F32)


def body(
    tok_h, gain_h, router_h, wg_h, wu_h, wd_h, rows_h, cnt_h,
    out_ref,
    tok, gain, router, wg, wu, wd, rows, cnt,
    picked, scaled, stat, stat_in, part, relay, ring, back, hidden, other, xcore, xcore_in, keep,
    summed, summed_in, updated, blocks, news, final, lasts, ready, final_in,
    load_sem, stat_s, stat_r, relay_s, relay_r, ring_s, ring_r, back_s, back_r, hid_s, hid_r,
    core_s, core_r, sum_s, sum_r, hop_s, blk_s, fwd_s, blk_r, fin_s, fin_r,
):
    sec = lax.axis_index("section")
    tp = lax.axis_index("tp")
    core = lax.rem(sec, 2)
    group = sec // 16
    chip = lax.rem(sec, 16) // 2
    ahead = lax.rem(tp + 1 + 2 * core, 4)
    behind = lax.rem(tp + 3 + 2 * core, 4)
    across = lax.rem(tp + 2, 4)
    sibling = sec + 1 - 2 * core
    sections, tps = 32, 4

    barrier = pltpu.get_barrier_semaphore()

    @pl.loop(1, sections)
    def _(k):
        pl.semaphore_signal(
            barrier, inc=1, device_id={"section": lax.rem(sec + k, sections), "tp": tp}, device_id_type=MESH
        )

    for k in range(1, tps):
        pl.semaphore_signal(
            barrier, inc=1, device_id={"section": sec, "tp": lax.rem(tp + k, tps)}, device_id_type=MESH
        )

    loads = []

    def load(src, dst):
        copy = pltpu.make_async_copy(src, dst, load_sem.at[len(loads)])
        copy.start()
        loads.append(copy)
        return copy

    small = [load(rows_h, rows), load(cnt_h, cnt), load(gain_h, gain), load(router_h, router)]
    tok_load = [load(tok_h.at[0], tok.at[0])]
    wgu_load = []
    for start, n in CHUNKS:
        cols = pl.ds(start, n)
        wgu_load.append(
            (load(wg_h.at[0, :, cols], wg.at[:, cols]), load(wu_h.at[0, :, cols], wu.at[:, cols]))
        )
    tok_load.append(load(tok_h.at[1], tok.at[1]))
    wd_load = load(wd_h.at[0], wd)

    @pl.loop(0, MICRO)
    def _(m):
        part[m, tps - 1, CAP - GROUP * (tps - 1) :, :] = jnp.zeros((GROUP * tps - CAP, 2 * HID), BF16)

    def remote(src, dst, ss, rs, section=None, z=None):
        return pltpu.make_async_remote_copy(
            src_ref=src,
            dst_ref=dst,
            send_sem=ss,
            recv_sem=rs,
            device_id={"section": sec if section is None else section, "tp": tp if z is None else z},
            device_id_type=MESH,
        )

    def routed(m, k):
        ids = rows[m, k : k + 1, :].astype(F32)
        count = cnt[m : m + 1, k : k + 1]
        return ids, iota((1, CAP), 1) < count

    owner = chip < BLOCKS
    my_block = BLOCKS * core + chip
    my_columns = pl.ds(pl.multiple_of(128 * jnp.minimum(my_block, 2 * BLOCKS - 1), 128), 128)

    def run(layer):
        sends = []

        def send(copy):
            copy.start()
            sends.append((None, copy))

        def base(m):
            if m == 0:
                for copy in small:
                    copy.wait()
            tok_load[m].wait()
            ids, live = routed(m, layer)
            column = as_column(ids)
            old = column == iota((CAP, TOK), 1).astype(F32)
            if layer == 1:
                ids0, live0 = routed(m, 0)
                new = column == jnp.where(live0, ids0, -2.0)
                old = old & (jnp.sum(jnp.where(new, 1.0, 0.0), axis=1, keepdims=True) < 0.5)
                news[m] = onehot(new)
            old = onehot(old)
            for b in range(Q // 256):
                cols = pl.ds(256 * b, 256)
                picked[m, :, cols] = dot(old, tok[m, :, cols]).astype(BF16)

        def pick(m):
            squares = jnp.zeros((CAP, 256), F32)
            logits = jnp.zeros((CAP, 256), F32)
            for b in range(Q // 256):
                cols = pl.ds(256 * b, 256)
                values = picked[m, :, cols].astype(F32)
                if layer == 1:
                    both = jnp.concatenate([blocks[m, 2 * b], blocks[m, 2 * b + 1]], axis=1)
                    values = values + dot(news[m], both)
                    picked[m, :, cols] = values.astype(BF16)
                squares = squares + values * values
                logits = logits + values * router[layer : layer + 1, cols]
                scaled[m, :, cols] = (values * gain[layer : layer + 1, cols]).astype(BF16)
            squares = as_row(jnp.sum(squares, axis=1, keepdims=True))
            logits = as_row(jnp.sum(logits, axis=1, keepdims=True))
            which = iota((8, CAP), 0)
            stat[m] = jnp.where(which == 0, squares, jnp.where(which == 1, logits, 0.0))

        def stat_copy(m, k):
            return remote(stat.at[m], stat_in.at[m, k - 1], stat_s.at[m, k - 1], stat_r.at[m, k - 1], z=lax.rem(tp + k, tps))

        def send_stats(m):
            for k in range(1, tps):
                send(stat_copy(m, k))

        def spans(n):
            start, width = CHUNKS[n]
            return pl.ds(2 * start, 2 * width), 2 * start, width

        def relay_copy(m, n):
            cols = spans(n)[0]
            return remote(part.at[m, across, :, cols], relay.at[m, :, cols], relay_s.at[m, n], relay_r.at[m, n], z=ahead)

        def back_copy(m, n):
            cols = spans(n)[0]
            return remote(part.at[m, behind, :, cols], back.at[m, :, cols], back_s.at[m, n], back_r.at[m, n], z=behind)

        def ring_copy(m, n):
            cols = spans(n)[0]
            return remote(ring.at[m, 0, :, cols], ring.at[m, 1, :, cols], ring_s.at[m, n], ring_r.at[m, n], z=ahead)

        def store_part(m, first, width, value):
            full = GROUP * (tps - 1)
            part[m, : tps - 1, :, first : first + width] = value[:full].reshape(tps - 1, GROUP, width)
            part[m, tps - 1, : CAP - full, first : first + width] = value[full:]

        def project(m, n):
            start, width = CHUNKS[n]
            if m == 0:
                wgu_load[n][0].wait()
            x = scaled[m]
            gate = dot(x, wg[:, start : start + width]).astype(BF16)
            store_part(m, 2 * start, width, gate)
            if m == 0:
                wgu_load[n][1].wait()
            up = dot(x, wu[:, start : start + width]).astype(BF16)
            store_part(m, 2 * start + width, width, up)

        def launch(m, n):
            if n == 0:
                send_stats(m)
            send(relay_copy(m, n))
            send(back_copy(m, n))

        def pass_on(m, n):
            cols = spans(n)[0]
            relay_copy(m, n).wait_recv()
            ring[m, 0, :, cols] = (part[m, ahead, :, cols].astype(F32) + relay[m, :, cols].astype(F32)).astype(BF16)
            send(ring_copy(m, n))

        def total_stats(m):
            return stat[m] + stat_in[m, 0] + stat_in[m, 1] + stat_in[m, 2]

        def hidden_copy(m, n, k):
            start, width = CHUNKS[n]
            mine = hidden.at[m, tp, :, pl.ds(start, width)]
            return remote(mine, mine, hid_s.at[m, n, k - 1], hid_r.at[m, n, k - 1], z=lax.rem(tp + k, tps))

        def activate(m, n):
            cols, first, width = spans(n)
            start = CHUNKS[n][0]
            if n == 0:
                for k in range(1, tps):
                    stat_copy(m, k).wait_recv()
            back_copy(m, n).wait_recv()
            ring_copy(m, n).wait_recv()
            inverse = lax.rsqrt(as_column(total_stats(m)[0:1], GROUP * tp, GROUP) / D + EPSILON)

            def values(at):
                c = pl.ds(at, width)
                return part[m, tp, :, c].astype(F32) + back[m, :, c].astype(F32) + ring[m, 1, :, c].astype(F32)

            gate = values(first) * inverse
            up = values(first + width) * inverse
            hidden[m, tp, :, start : start + width] = (gate / (1.0 + jnp.exp(-gate)) * up).astype(BF16)
            for k in (2, 1, 3):
                send(hidden_copy(m, n, k))

        def core_copy(m):
            return remote(xcore.at[m], xcore_in.at[m], core_s.at[m], core_r.at[m], section=sibling)

        def down(m, n):
            for k in range(1, tps):
                hidden_copy(m, n, k).wait_recv()
            if m == 0 and n == 0:
                wd_load.wait()
            start, width = CHUNKS[n]
            units = slice(start, start + width)
            x = hidden[m, :, :, units].reshape(GROUP * tps, width)[:CAP]
            theirs = dot(x, wd[units, pl.ds(pl.multiple_of(HALF * (1 - core), 128), HALF)])
            if n == 0:
                other[m] = theirs
            else:
                xcore[m] = (other[m] + theirs).astype(BF16)
                send(core_copy(m))
            mine = dot(x, wd[units, pl.ds(pl.multiple_of(HALF * core, 128), HALF)])
            if n == 0:
                keep[m] = mine
            else:
                keep[m] += mine

        def sum_copy(m, k):
            there = lax.rem(chip + k, 8)
            return there < BLOCKS, remote(
                summed.at[m, there], summed_in.at[m, k - 1], sum_s.at[m, k - 1], sum_r.at[m, k - 1],
                section=16 * group + 2 * there + core,
            )

        def send_if(condition, copy):
            @pl.when(condition)
            def _():
                copy.start()

            sends.append((condition, copy))

        def spread(m):
            core_copy(m).wait_recv()
            for b in range(BLOCKS):
                cols = pl.ds(128 * b, 128)
                summed[m, b] = (keep[m, :, cols] + xcore_in[m, :, cols].astype(F32)).astype(BF16)
            for k in range(1, 8):
                there = lax.rem(chip + k, 8)

                @pl.when(there < BLOCKS)
                def _():
                    sum_copy(m, k)[1].start()

                sends.append((there < BLOCKS, sum_copy(m, k)[1]))


        def hop_copy(m):
            return remote(
                updated.at[m], blocks.at[m, my_block], hop_s.at[m], blk_r.at[m, my_block],
                section=16 + 2 * lax.rem(chip + 4, 8) + core,
            )

        def combine(m):
            @pl.when(owner)
            def _():
                total = summed[m, chip].astype(F32)
                for k in range(1, 8):
                    sum_copy(m, k)[1].wait_recv()
                    total = total + summed_in[m, k - 1].astype(F32)
                logits = as_column(total_stats(m)[1:2])
                gate = 1.0 / (1.0 + jnp.exp(-logits))
                updated[m] = (picked[m, :, my_columns].astype(F32) + gate * total).astype(BF16)

                if layer == 0:
                    hop_copy(m).start()

            if layer == 0:
                sends.append((owner, hop_copy(m)))

        source = lax.rem(chip + 4, 8)
        has_block = source < BLOCKS

        def block_copy(m, k):
            block = BLOCKS * core + source
            return remote(
                blocks.at[m, block], blocks.at[m, block], blk_s.at[m, k - 1], blk_r.at[m, block],
                section=16 + 2 * lax.rem(chip + k, 8) + core,
            )

        def forward_copy(m, k):
            block = BLOCKS * core + lax.rem(source + k, 8)
            return remote(
                blocks.at[m, block], blocks.at[m, block], fwd_s.at[m, k], blk_r.at[m, block], section=sibling
            )

        def arrival(m, block):
            return remote(blocks.at[m, block], blocks.at[m, block], fwd_s.at[m, 0], blk_r.at[m, block], section=sibling)

        def broadcast(m):
            @pl.when(has_block)
            def _():
                arrival(m, BLOCKS * core + source).wait_recv()
                for k in range(1, 8):
                    block_copy(m, k).start()
                forward_copy(m, 0).start()

            for k in range(1, 8):
                sends.append((has_block, block_copy(m, k)))
            sends.append((has_block, forward_copy(m, 0)))

        def forward(m):
            for k in (1, 7, 4, 5, 3, 2, 6):
                there = lax.rem(source + k, 8)

                @pl.when(there < BLOCKS)
                def _():
                    arrival(m, BLOCKS * core + there).wait_recv()
                    forward_copy(m, k).start()

            for b in range(BLOCKS):
                arrival(m, BLOCKS * (1 - core) + b).wait_recv()

            for k in range(1, 8):
                sends.append((lax.rem(source + k, 8) < BLOCKS, forward_copy(m, k)))

        def finish(m):
            @pl.when(owner)
            def _():
                r = iota((16 * sections, 1), 0)
                i = r & 7
                token = jnp.where((((r >> 3) & 1) == m) & (i < OWN_TOKENS), OWN_TOKENS * (r >> 4) + i, -5).astype(F32)

                def matches(k):
                    ids, live = routed(m, k)
                    return token == jnp.where(live, ids, -1.0)

                def any_of(hit):
                    return jnp.sum(jnp.where(hit, 1.0, 0.0), axis=1, keepdims=True) > 0.5

                last = matches(1)
                in_last = any_of(last)
                first = matches(0)
                in_first = any_of(first)
                base = token == iota((16 * sections, TOK), 1).astype(F32)
                value = dot(onehot(base & ~(in_first | in_last)), tok[m, :, my_columns])
                value = value + dot(onehot(first & ~in_last), blocks[m, my_block])
                if m == 0:
                    final[...] = value + dot(onehot(last), updated[m])
                else:
                    final[...] += value
                    lasts[...] = onehot(last)

        def final_copy(k, dy, dx, dc):
            row, column = lax.rem(sec // 8 + dy, 4), lax.rem(chip + dx, 4)
            there = 8 * row + 2 * column + (core if dc == 0 else 1 - core)
            return remote(ready.at[there], final_in.at[my_block], fin_s.at[k], fin_r.at[my_block], section=there)

        def final_copies():
            steps = [(dy, dx, dc) for dy in range(4) for dx in range(4) for dc in range(2)]
            steps.sort(key=lambda o: -(min(o[0], 4 - o[0]) + min(o[1], 4 - o[1])))
            steps.remove((0, 0, 0))
            return [final_copy(k, *step) for k, step in enumerate(steps)]

        def arrived(b):
            remote(ready.at[0], final_in.at[b], fin_s.at[0], fin_r.at[b], section=sibling).wait_recv()

        def deliver():
            if layer == 1:

                @pl.when(owner)
                def _():
                    value = final[...] + dot(lasts[...], updated[MICRO - 1])
                    ready[...] = value.astype(BF16).reshape(sections, 16, 128)

                    for copy in final_copies():
                        copy.start()

                    final_in[my_block] = ready[sec]

            for b in range(2 * BLOCKS):
                if layer == 1:
                    pl.when(jnp.logical_not(owner & (my_block == b)))(functools.partial(arrived, b))
                else:
                    arrived(b)
                for m in range(MICRO):
                    out_ref[:, m, 128 * b : 128 * b + 128] = final_in[b, 8 * m : 8 * m + OWN_TOKENS, :]

        def enter():
            pl.semaphore_wait(barrier, sections + tps - 2)

        orders = (
            (
                (base, 0), (pick, 0), (project, 0, 0), (enter,), (launch, 0, 0), (project, 0, 1), (launch, 0, 1),
                (base, 1), (pick, 1), (project, 1, 0), (project, 1, 1), (pass_on, 0, 0), (pass_on, 0, 1),
                (launch, 1, 0), (activate, 0, 0), (launch, 1, 1), (activate, 0, 1), (pass_on, 1, 0), (pass_on, 1, 1),
                (down, 0, 0), (activate, 1, 0), (down, 0, 1), (spread, 0), (activate, 1, 1), (down, 1, 0),
                (combine, 0), (down, 1, 1), (spread, 1), (combine, 1), (deliver,),
            ),
            (
                (enter,), (base, 0), (base, 1), (broadcast, 0), (forward, 0), (pick, 0), (project, 0, 0),
                (launch, 0, 0), (project, 0, 1), (launch, 0, 1), (broadcast, 1), (pass_on, 0, 0), (pass_on, 0, 1),
                (activate, 0, 0), (forward, 1), (pick, 1), (activate, 0, 1), (project, 1, 0), (launch, 1, 0),
                (project, 1, 1), (launch, 1, 1), (down, 0, 0), (pass_on, 1, 0), (down, 0, 1), (pass_on, 1, 1),
                (spread, 0), (activate, 1, 0), (activate, 1, 1), (down, 1, 0), (combine, 0), (down, 1, 1),
                (spread, 1), (finish, 0), (finish, 1), (combine, 1), (deliver,),
            ),
        )
        for task, *which in orders[layer]:
            with jax.named_scope("_".join([task.__name__, *map(str, which)])):
                task(*which)

        def drain():
            for condition, copy in sends:
                if condition is None:
                    copy.wait_send()
                else:
                    pl.when(condition)(copy.wait_send)

            if layer == 1:

                @pl.when(owner)
                def _():
                    for copy in final_copies():
                        copy.wait_send()

        with jax.named_scope("drain"):
            drain()

    for layer in range(2):
        pl.when(group == layer)(functools.partial(run, layer))


def on_device(*args):
    return jnp.swapaxes(call(*args), 0, 1)


def call(*args):
    dma = pltpu.SemaphoreType.DMA
    n = len(CHUNKS)
    return pl.pallas_call(
        body,
        out_shape=pltpu.VMEM((OWN_TOKENS, MICRO, Q), BF16),
        in_specs=[pl.BlockSpec(memory_space=pl.ANY)] * 8,
        out_specs=pl.BlockSpec(memory_space=pltpu.VMEM),
        scratch_shapes=[
            pltpu.VMEM((MICRO, TOK, Q), BF16),
            pltpu.VMEM((2, Q), F32),
            pltpu.VMEM((2, Q), F32),
            pltpu.VMEM((Q, HID), BF16),
            pltpu.VMEM((Q, HID), BF16),
            pltpu.VMEM((HID, Q), BF16),
            pltpu.VMEM((MICRO, 2, CAP), jnp.int32),
            pltpu.VMEM((MICRO, 2), jnp.int32),
            pltpu.VMEM((MICRO, CAP, Q), BF16),
            pltpu.VMEM((MICRO, CAP, Q), BF16),
            pltpu.VMEM((MICRO, 8, CAP), F32),
            pltpu.VMEM((MICRO, 3, 8, CAP), F32),
            pltpu.VMEM((MICRO, 4, 32, 2 * HID), BF16),
            pltpu.VMEM((MICRO, 32, 2 * HID), BF16),
            pltpu.VMEM((MICRO, 2, 32, 2 * HID), BF16),
            pltpu.VMEM((MICRO, 32, 2 * HID), BF16),
            pltpu.VMEM((MICRO, 4, 32, HID), BF16),
            pltpu.VMEM((MICRO, CAP, HALF), F32),
            pltpu.VMEM((MICRO, CAP, HALF), BF16),
            pltpu.VMEM((MICRO, CAP, HALF), BF16),
            pltpu.VMEM((MICRO, CAP, HALF), F32),
            pltpu.VMEM((MICRO, 8, CAP, 128), BF16),
            pltpu.VMEM((MICRO, 7, CAP, 128), BF16),
            pltpu.VMEM((MICRO, CAP, 128), BF16),
            pltpu.VMEM((MICRO, 2 * BLOCKS + 1, CAP, 128), BF16),
            pltpu.VMEM((MICRO, CAP, CAP), BF16),
            pltpu.VMEM((512, 128), F32),
            pltpu.VMEM((512, CAP), BF16),
            pltpu.VMEM((32, 16, 128), BF16),
            pltpu.VMEM((2 * BLOCKS + 1, 16, 128), BF16),
            dma((6 + 2 * n + 1,)),
            dma((MICRO, 3)), dma((MICRO, 3)),
            dma((MICRO, n)), dma((MICRO, n)),
            dma((MICRO, n)), dma((MICRO, n)),
            dma((MICRO, n)), dma((MICRO, n)),
            dma((MICRO, n, 3)), dma((MICRO, n, 3)),
            dma((MICRO,)), dma((MICRO,)),
            dma((MICRO, 7)), dma((MICRO, 7)),
            dma((MICRO,)),
            dma((MICRO, 7)),
            dma((MICRO, 8)),
            dma((MICRO, 2 * BLOCKS + 1)),
            dma((31,)),
            dma((2 * BLOCKS + 1,)),
        ],
        compiler_params=pltpu.CompilerParams(
            collective_id=0, has_side_effects=True, vmem_limit_bytes=60 * 1024 * 1024
        ),
        name="layers",
    )(*args)


def solution(mesh):
    return jax.shard_map(
        on_device,
        mesh=mesh,
        in_specs=(
            P(None, None, "tp"),
            P(None, "tp"),
            P(None, "tp"),
            P("section", "tp", None),
            P("section", "tp", None),
            P("section", None, "tp"),
            P(),
            P(),
        ),
        out_specs=P(None, "section", "tp"),
        check_vma=False,
    )
```
